128 devices in a mesh: seg: 32 (over y_lo, x, z), rep: 4 (over y_hi, core).
Axes of the slice: x: 4, y: 4 (y_hi: 2, y_lo: 2; y = y_hi * 2 + y_lo), z: 4, core: 2. Of those that a mesh axis runs over, the one named last changes fastest.
Arguments:
- decoder_rows: bfloat16 [256, 4096], P('rep', 'seg'), may hold values from -2000 to 2000
- norm_gain: float32 [4096], replicated, may hold values from 0.5 to 1.5
- query_weight: bfloat16 [4096, 4096], P('rep', 'seg'), may hold values from -1 to 1
- key_codes: bfloat16 [4, 16384, 4096], P('rep', 'seg'), may hold values from -127 to 127, as said below
- key_scale: float32 [4, 128, 64], P('rep', 'seg'), may hold values from 0.5 to 1.5
- value_codes: bfloat16 [4, 16384, 4096], P('rep', 'seg'), may hold values from -6 to 6
- value_scale: float32 [4, 128, 64], P('rep', 'seg'), may hold values from 0.5 to 2
- enc_lengths: int32 [4], P('rep'), may hold values from 4096 to 16384
- output_weight: bfloat16 [4096, 4096], P('seg', 'rep'), may hold values from -0.09375 to 0.09375
Outputs:
- update: bfloat16 [256, 4096], P('rep', 'seg')
The draws below stay inside these ranges and needn't reach their ends.
Inputs may be any that keep to these rules, and one draw needn't show every extreme that they name: `key_codes`: codes of a block times its scale give the cached keys.
All inputs are finite; a program needn't handle non-finite values.
Results may differ from the reference program's by a relative error of at most 0.011.
Values may be sent and summed in bfloat16 or wider, within the bound.
No kernel may reach another device: no remote copies, remote signals or barrier semaphores. Data moves between devices by JAX's collectives and lax.ppermute only.
A program may use at most 64 MiB of HBM per device.

```python
import math
import jax
import jax.numpy as jnp
from jax import lax

D = 4096
HEADS = 64
HEAD_DIM = 64
QRY = 64
SCALE_GROUP = 128
INNER = 4096
DOCS = 4
ROWS = 256
ENC = 16384
NBLK = 128


def row_values(key):
    base_key = jax.random.fold_in(key, 101)
    key_row, key_col, key_base = jax.random.split(base_key, 3)
    row_factor = jnp.exp(jax.random.uniform(key_row, (ROWS, 1), jnp.float32) * math.log(10.0))
    col_rise = jnp.exp(jnp.arange(D, dtype=jnp.float32) / D * math.log(3.0))[None, :]
    col_factor = jnp.exp(jax.random.uniform(key_col, (1, D), jnp.float32) * math.log(10.0)) * col_rise
    base = jnp.clip(jax.random.normal(key_base, (ROWS, D), jnp.float32), -6.0, 6.0)
    return base * row_factor * col_factor


def gain_values(key):
    gain_key = jax.random.fold_in(key, 202)
    return 1.0 + jnp.clip(0.1 * jax.random.normal(gain_key, (D,), jnp.float32), -0.45, 0.45)


def weight_values(key):
    weight_key = jax.random.fold_in(key, 303)
    base = jnp.clip(jax.random.normal(weight_key, (D, INNER), jnp.float32), -6.0, 6.0)
    return base / math.sqrt(D)


def draw_decoder_rows(key, part):
    return row_values(key).astype(jnp.bfloat16)


def draw_norm_gain(key, part):
    return gain_values(key)


def draw_query_weight(key, part):
    return weight_values(key).astype(jnp.bfloat16)


def draw_key_codes(key, part):
    code_key = jax.random.fold_in(key, 404)
    key_base = jax.random.fold_in(code_key, 0)
    codes = jnp.clip(0.4 * jax.random.normal(key_base, (DOCS, ENC, INNER), jnp.float32), -3.2, 3.2)
    return codes.astype(jnp.bfloat16)


def place_ends(entries, key, smallest, high):
    dims = entries.shape
    spot = [jax.random.randint(jax.random.fold_in(key, axis), (), 0, dims[axis]) for axis in range(len(dims))]
    entries = entries.at[tuple(spot)].set(smallest)
    longest = dims.index(max(dims))
    spot[longest] = (spot[longest] + 1) % dims[longest]
    return entries.at[tuple(spot)].set(high)


def level_of(rng, shape, pieces, least, largest):
    def one(position, shards_of):
        heights = jax.random.uniform(jax.random.fold_in(jax.random.fold_in(rng, 6), position), (shards_of,), jnp.float32, least / len(pieces), largest / len(pieces))
        return jnp.repeat(jnp.exp(heights), shape[position] // shards_of).reshape((-1,) + (1,) * (len(shape) - position - 1))

    factor_of = one(*pieces[0])
    for cut in pieces[1:]:
        factor_of = factor_of * one(*cut)
    return factor_of


def normal_values(stream_key, shape, scale, bound, cuts=(), held_as=jnp.bfloat16):
    gain = level_of(stream_key, shape, cuts, -0.22, 0.18) if cuts else 1.0
    values = jax.random.normal(stream_key, shape, jnp.float32) * scale * gain
    return jnp.minimum(jnp.maximum(values, -bound), bound).astype(held_as)


def setup_inputs(seed: int = 0) -> dict:
    key_of = jax.random.split(jax.random.key(seed), 10)
    decoder_rows = draw_decoder_rows(jax.random.fold_in(key_of[9], 71), 0)
    norm_gain = draw_norm_gain(jax.random.fold_in(key_of[9], 71), 0)
    query_weight = draw_query_weight(jax.random.fold_in(key_of[9], 71), 0)
    key_codes = draw_key_codes(jax.random.fold_in(key_of[9], 71), 0)
    key_scale = jnp.clip(jnp.exp(math.log(1.5) - 1.0986123 * jax.random.uniform(key_of[4], (DOCS, NBLK, HEADS), jnp.float32) ** level_of(key_of[4], (DOCS, NBLK, HEADS), ((0, 4), (1, 32)), -0.2, 0.2)), 0.5, 1.5)
    value_codes = normal_values(key_of[5], (DOCS, ENC, INNER), 1.0, 6.0, ((0, 4), (1, 32)))
    value_scale = jnp.clip(jnp.exp(math.log(2.0) - 1.3862944 * jax.random.uniform(key_of[6], (DOCS, NBLK, HEADS), jnp.float32) ** level_of(key_of[6], (DOCS, NBLK, HEADS), ((0, 4), (1, 32)), -0.2, 0.2)), 0.5, 2.0)
    enc_lengths = place_ends(jax.random.randint(key_of[7], (DOCS,), ENC // 4, ENC + 1), jax.random.fold_in(key_of[7], 1), ENC // 4, ENC).astype(jnp.int32)
    output_weight = normal_values(key_of[8], (INNER, D), INNER ** -0.5, 0.09375, ((0, 32), (1, 4)))
    return dict(decoder_rows=decoder_rows, norm_gain=norm_gain, query_weight=query_weight, key_codes=key_codes, key_scale=key_scale, value_codes=value_codes, value_scale=value_scale, enc_lengths=enc_lengths, output_weight=output_weight)


def attend_document(document_query, document_keys, document_values, document_key_scale, document_value_scale, document_length):
    query_for_head = document_query.reshape(QRY, HEADS, HEAD_DIM).transpose(1, 0, 2)
    keys_for_head = document_keys.reshape(ENC, HEADS, HEAD_DIM).transpose(1, 0, 2)
    values_for_head = document_values.reshape(ENC, HEADS, HEAD_DIM).transpose(1, 0, 2)
    usable = (jnp.arange(ENC, dtype=jnp.int32) < document_length)[None, :]

    def single_head(group_members):
        query_of_head, key_of_head, value_of_head, key_scale_of_head, value_scale_of_head = group_members
        attention_scores = jnp.dot(query_of_head, key_of_head.T, preferred_element_type=jnp.float32)
        attention_scores = attention_scores * jnp.repeat(key_scale_of_head, SCALE_GROUP)[None, :]
        attention_scores = jnp.where(usable, attention_scores, jnp.float32(-1e+30))
        peaks = lax.optimization_barrier(jnp.max(attention_scores, axis=-1, keepdims=True))
        weights = jnp.where(usable, jnp.exp(attention_scores - peaks), jnp.float32(0.0))
        totals = lax.optimization_barrier(jnp.sum(weights, axis=-1, keepdims=True))
        scaled = (weights * jnp.repeat(value_scale_of_head, SCALE_GROUP)[None, :]).astype(jnp.bfloat16)
        summed = jnp.dot(scaled, value_of_head, preferred_element_type=jnp.float32)
        return (summed / totals).astype(jnp.bfloat16)
    each_head_output = lax.map(single_head, (query_for_head, keys_for_head, values_for_head, document_key_scale.T, document_value_scale.T))
    return each_head_output.transpose(1, 0, 2).reshape(QRY, INNER)

def reference(decoder_rows, norm_gain, query_weight, key_codes, key_scale, value_codes, value_scale, enc_lengths, output_weight):
    widened = decoder_rows.astype(jnp.float32)
    variance = lax.optimization_barrier(jnp.mean(widened * widened, axis=-1, keepdims=True))
    normed = (widened * lax.rsqrt(variance + 1e-06) * norm_gain[None, :]).astype(jnp.bfloat16)
    queries = jnp.dot(normed, query_weight, preferred_element_type=jnp.float32).astype(jnp.bfloat16)
    attended_docs = []
    for doc_index in range(DOCS):
        document_query = queries[doc_index * QRY:(doc_index + 1) * QRY]
        attended_docs.append(attend_document(document_query, key_codes[doc_index], value_codes[doc_index], key_scale[doc_index], value_scale[doc_index], enc_lengths[doc_index]))
    attended = jnp.concatenate(attended_docs, axis=0)
    return jnp.dot(attended, output_weight, preferred_element_type=jnp.float32).astype(jnp.bfloat16)
```

```python
import functools
import math

import jax
import jax.numpy as jnp
from jax import lax
from jax.experimental import pallas as pl
from jax.experimental.pallas import tpu as pltpu
from jax.sharding import PartitionSpec as P

LOG2E = math.log2(math.e)
BF16, F32 = jnp.bfloat16, jnp.float32
LANES = 128
STAT_ROWS = 8
EMPTY = -1e30
VMEM = pl.BlockSpec(memory_space=pltpu.VMEM)
SMEM = pl.BlockSpec(memory_space=pltpu.SMEM)


def params(mib):
    return pltpu.CompilerParams(vmem_limit_bytes=mib << 20)


def cost(flops, moved):
    return pl.CostEstimate(flops=flops, bytes_accessed=moved, transcendentals=0)


def flip_pair(block):
    half = block.shape[0]
    turned = jnp.concatenate([block, block], axis=0).T
    left = lax.broadcasted_iota(jnp.int32, block.shape, 1) < half
    return jnp.where(left, turned[:half], turned[half:])


def query_kernel(rep_ref, x_ref, gain_ref, *refs):
    weights, out_ref = refs[:-1], refs[-1]
    segs, rows, _ = x_ref.shape
    each = segs // len(weights)
    squares = jnp.zeros((rows, LANES), F32)
    for j in range(segs):
        wide = x_ref[j].astype(F32)
        squares += wide * wide
    mean = jnp.sum(squares, axis=1, keepdims=True) * (1.0 / (segs * LANES))
    scale = lax.rsqrt(mean + 1e-06)
    total = jnp.zeros((rows, LANES), F32)
    for i, w_ref in enumerate(weights):
        first = (rep_ref[0] ^ i) * each
        for j in range(0, each, 2):
            pair = [
                (x_ref[first + k].astype(F32) * scale * gain_ref[pl.ds(first + k, 1), :]).astype(BF16)
                for k in (j, j + 1)
            ]
            total += jnp.dot(
                jnp.concatenate(pair, axis=1),
                w_ref[j * LANES : (j + 2) * LANES, :],
                preferred_element_type=F32,
            )
    own = flip_pair(total).astype(BF16)
    for j in range(segs):
        out_ref[j] = own


def turn_kernel(v_ref, out_ref):
    out_ref[...] = v_ref[...].T


def attend_kernel(used_ref, q_ref, k_ref, vt_ref, ks_ref, vs_ref, out_ref):
    segs = q_ref.shape[0]
    half = q_ref.shape[1]
    tokens = k_ref.shape[0]
    blocks = ks_ref.shape[0]
    each = tokens // blocks
    wide = 2 * LANES
    used = used_ref[0]
    sub = lax.broadcasted_iota(jnp.int32, (STAT_ROWS, LANES), 0)
    left = lax.broadcasted_iota(jnp.int32, (half, LANES), 1) < half

    def put(pair, sums, log_sum):
        out_ref[pair, 0:half, :] = sums.astype(BF16)
        high = log_sum.astype(BF16).astype(F32)
        mid = (log_sum - high).astype(BF16).astype(F32)
        low = log_sum - high - mid
        stats = jnp.where(sub == 0, high, jnp.where(sub == 1, mid, jnp.where(sub == 2, low, 0.0)))
        out_ref[pair, half : half + STAT_ROWS, :] = stats.astype(BF16)

    @pl.when(used <= 0)
    def _():
        for pair in range(segs):
            put(pair, jnp.zeros((half, LANES), F32), jnp.full((1, LANES), EMPTY, F32))

    @pl.when(used > 0)
    def _():
        def group(g, carry):
            lanes = pl.ds(pl.multiple_of(g * wide, wide), wide)
            none = jnp.zeros((half, LANES), BF16)
            q0, q1 = q_ref[2 * g], q_ref[2 * g + 1]
            placed = jnp.concatenate(
                [
                    jnp.concatenate([jnp.where(left, q0, none), none], axis=1),
                    jnp.concatenate([jnp.where(left, none, q0), none], axis=1),
                    jnp.concatenate([none, jnp.where(left, q1, none)], axis=1),
                    jnp.concatenate([none, jnp.where(left, none, q1)], axis=1),
                ],
                axis=0,
            )
            scores = []
            for b in range(blocks):
                part = jnp.dot(
                    k_ref[b * each : (b + 1) * each, lanes], placed, preferred_element_type=F32
                )
                part = part * ks_ref[b : b + 1, lanes]
                place = b * each + lax.broadcasted_iota(jnp.int32, part.shape, 0)
                scores.append(jnp.where(place < used, part, EMPTY))
            peak = functools.reduce(jnp.maximum, [jnp.max(p, axis=0, keepdims=True) for p in scores])
            total = jnp.zeros((1, wide), F32)
            scaled = []
            for b in range(blocks):
                weight = jnp.exp2(scores[b] - peak)
                total += jnp.sum(weight, axis=0, keepdims=True)
                scaled.append((weight * vs_ref[b : b + 1, lanes]).astype(BF16))
            sums = jnp.dot(
                vt_ref[pl.ds(pl.multiple_of(g * wide, wide), wide), :],
                jnp.concatenate(scaled, axis=0),
                preferred_element_type=F32,
            )
            inverse = 1.0 / total
            log_sum = peak + jnp.log2(total)
            for i in range(2):
                at = slice(i * LANES, (i + 1) * LANES)
                mine = jnp.where(
                    left,
                    sums[i * LANES : i * LANES + half, at],
                    sums[i * LANES + half : (i + 1) * LANES, at],
                )
                put(2 * g + i, mine * inverse[:, at], log_sum[:, at])
            return carry

        lax.fori_loop(0, segs // 2, group, 0)


def output_kernel(rep_ref, part_ref, *refs):
    weights, out_ref = refs[:-1], refs[-1]
    segs = part_ref.shape[0]
    half = part_ref.shape[1] - STAT_ROWS
    log_sum = jnp.sum(part_ref[:, half : half + STAT_ROWS, :].astype(F32), axis=1)
    share = jnp.exp2(log_sum - jnp.max(log_sum, axis=0, keepdims=True))
    share = share / jnp.sum(share, axis=0, keepdims=True)
    total = jnp.zeros((half, LANES), F32)
    for j in range(segs):
        total += part_ref[j, 0:half, :].astype(F32) * share[j : j + 1, :]
    attended = flip_pair(total).astype(BF16)
    each = segs // len(weights)
    for i, w_ref in enumerate(weights):
        first = (rep_ref[0] ^ i) * each
        update = jnp.dot(attended, w_ref[...], preferred_element_type=F32)
        for j in range(each):
            out_ref[first + j] = update[:, j * LANES : (j + 1) * LANES].astype(BF16)


def sum_kernel(part_ref, out_ref):
    total = part_ref[0].astype(F32)
    for j in range(1, part_ref.shape[0]):
        total += part_ref[j].astype(F32)
    out_ref[...] = total.astype(BF16)


def over_rep(block):
    core = [(0, 1), (1, 0), (2, 3), (3, 2)]
    chip = [(0, 2), (1, 3), (2, 0), (3, 1)]
    far = lax.ppermute(block, "rep", chip)
    near = lax.ppermute(block, "rep", core)
    return block, near, far, lax.ppermute(far, "rep", core)


def swapped(blocks):
    return lax.all_to_all(blocks, "seg", split_axis=0, concat_axis=0, tiled=True)


def per_device(
    decoder_rows,
    norm_gain,
    query_weight,
    key_codes,
    key_scale,
    value_codes,
    value_scale,
    enc_lengths,
    output_weight,
):
    segs = lax.axis_size("seg")
    rows, own = decoder_rows.shape
    _, tokens, inner = key_codes.shape
    blocks, heads = key_scale.shape[1:]
    head_dim = inner // heads
    rep = lax.axis_index("rep").astype(jnp.int32).reshape(1)
    used = jnp.clip(enc_lengths - lax.axis_index("seg") * tokens, 0, tokens).astype(jnp.int32)
    gain = norm_gain.reshape(segs, own)
    key_lanes = jnp.repeat(key_scale[0] * LOG2E, head_dim, axis=1)
    value_lanes = jnp.repeat(value_scale[0], head_dim, axis=1)

    query_blocks = over_rep(query_weight)
    x_all = swapped(jnp.broadcast_to(decoder_rows[None], (segs, rows, own)))
    query_sent = pl.pallas_call(
        query_kernel,
        out_shape=jax.ShapeDtypeStruct((segs, head_dim, LANES), BF16),
        in_specs=[SMEM] + [VMEM] * 6,
        out_specs=VMEM,
        compiler_params=params(16),
        cost_estimate=cost(2 * rows * inner * own, 2 << 20),
        name="query",
    )(rep, x_all, gain, *query_blocks)
    queries = swapped(query_sent)

    turn = 512
    values_t = pl.pallas_call(
        turn_kernel,
        grid=(inner // turn,),
        out_shape=jax.ShapeDtypeStruct((inner, tokens), BF16),
        in_specs=[pl.BlockSpec((tokens, turn), lambda i: (0, i))],
        out_specs=pl.BlockSpec((turn, tokens), lambda i: (i, 0)),
        compiler_params=params(16),
        cost_estimate=cost(2 * inner * tokens * 512, 8 << 20),
        name="turn",
    )(value_codes[0])

    parts = pl.pallas_call(
        attend_kernel,
        out_shape=jax.ShapeDtypeStruct((segs, head_dim + STAT_ROWS, LANES), BF16),
        in_specs=[SMEM] + [VMEM] * 5,
        out_specs=VMEM,
        compiler_params=params(28),
        cost_estimate=cost(16 * rows * inner * tokens, 9 << 20),
        name="attend",
    )(used, queries, key_codes[0], values_t, key_lanes, value_lanes)
    parts = swapped(parts)

    output_blocks = over_rep(output_weight)
    sent = pl.pallas_call(
        output_kernel,
        out_shape=jax.ShapeDtypeStruct((segs, rows, own), BF16),
        in_specs=[SMEM] + [VMEM] * 5,
        out_specs=VMEM,
        compiler_params=params(16),
        cost_estimate=cost(2 * rows * inner * own, 2 << 20),
        name="output",
    )(rep, parts, *output_blocks)
    return pl.pallas_call(
        sum_kernel,
        out_shape=jax.ShapeDtypeStruct((rows, own), BF16),
        in_specs=[VMEM],
        out_specs=VMEM,
        compiler_params=params(8),
        name="gather_sum",
    )(swapped(sent))


def solution(mesh):
    placed = (
        P("rep", "seg"),
        P(),
        P("rep", "seg"),
        P("rep", "seg", None),
        P("rep", "seg", None),
        P("rep", "seg", None),
        P("rep", "seg", None),
        P("rep"),
        P("seg", "rep"),
    )
    return jax.shard_map(
        per_device, mesh=mesh, in_specs=placed, out_specs=P("rep", "seg"), check_vma=False
    )
```

```python
import math

import jax
import jax.numpy as jnp
from jax import lax
from jax.experimental import pallas as pl
from jax.experimental.pallas import tpu as pltpu
from jax.sharding import PartitionSpec as P

LOG2E = math.log2(math.e)
BF16, F32 = jnp.bfloat16, jnp.float32
LANES = 128
STAT_ROWS = 8
SUM_ROWS = 16
EMPTY = -1e30
VMEM = pl.BlockSpec(memory_space=pltpu.VMEM)
SMEM = pl.BlockSpec(memory_space=pltpu.SMEM)
HBM = pl.BlockSpec(memory_space=pltpu.HBM)


def params(mib):
    return pltpu.CompilerParams(vmem_limit_bytes=mib << 20)


def cost(flops, moved):
    return pl.CostEstimate(flops=flops, bytes_accessed=moved, transcendentals=0)


def flip_pair(block):
    half = block.shape[0]
    turned = jnp.concatenate([block, block], axis=0).T
    left = lax.broadcasted_iota(jnp.int32, block.shape, 1) < half
    return jnp.where(left, turned[:half], turned[half:])


def stage_kernel(own_ref, gain_ref, own_out, gain_out):
    own_out[...] = own_ref[...]
    gain_out[...] = gain_ref[...]


def query_kernel(rep_ref, x_ref, gain_ref, *refs):
    weights, out_ref = refs[:-1], refs[-1]
    segs, rows, _ = x_ref.shape
    squares = jnp.zeros((rows, LANES), F32)
    for j in range(segs):
        wide = x_ref[j].astype(F32)
        squares += wide * wide
    mean = jnp.sum(squares, axis=1, keepdims=True) * (1.0 / (segs * LANES))
    scale = lax.rsqrt(mean + 1e-06)
    each = segs // len(weights)
    total = jnp.zeros((rows, LANES), F32)
    for i, w_ref in enumerate(weights):
        first = (rep_ref[0] ^ i) * each
        for j in range(0, each, 2):
            pair = [
                (x_ref[first + k].astype(F32) * scale * gain_ref[pl.ds(first + k, 1), :]).astype(BF16)
                for k in (j, j + 1)
            ]
            total += jnp.dot(
                jnp.concatenate(pair, axis=1),
                w_ref[j * LANES : (j + 2) * LANES, :],
                preferred_element_type=F32,
            )
    own = flip_pair(total).astype(BF16)
    for j in range(segs):
        out_ref[j] = own


def turn_kernel(v_ref, out_ref):
    turned = v_ref[...].T
    shape = (SUM_ROWS, turned.shape[1])
    row = lax.broadcasted_iota(jnp.int32, shape, 0)
    block = lax.broadcasted_iota(jnp.int32, shape, 1) // LANES
    picks = jnp.where(row == block, 1.0, 0.0).astype(BF16)
    for i in range(2):
        out_ref[0, i, 0:LANES, :] = turned[i * LANES : (i + 1) * LANES]
        out_ref[0, i, LANES : LANES + SUM_ROWS, :] = picks


def attend_kernel(
    used_ref, q_ref, ks_ref, lvs_ref, ivs_ref, k_hbm, vt_hbm, out_ref,
    k_buf, vt_buf, s0, s1, p0, p1, m0, m1, n0, n1, k_sems, vt_sems,
):
    groups = vt_hbm.shape[0]
    half = q_ref.shape[1]
    blocks = ks_ref.shape[0]
    wide = 2 * LANES
    used = used_ref[0]
    sub = lax.broadcasted_iota(jnp.int32, (STAT_ROWS, LANES), 0)
    left = lax.broadcasted_iota(jnp.int32, (half, LANES), 1) < half

    def lanes_of(g):
        return pl.ds(g * wide if isinstance(g, int) else pl.multiple_of(g * wide, wide), wide)

    def k_copy(g):
        return pltpu.make_async_copy(k_hbm.at[:, lanes_of(g)], k_buf.at[g], k_sems.at[g])

    def vt_copy(g):
        return pltpu.make_async_copy(vt_hbm.at[g], vt_buf.at[g], vt_sems.at[g])

    for g in range(groups):
        k_copy(g).start()
        vt_copy(g).start()

    def put(pair, sums, log_sum):
        out_ref[pair, 0:half, :] = sums.astype(BF16)
        high = log_sum.astype(BF16).astype(F32)
        mid = (log_sum - high).astype(BF16).astype(F32)
        low = log_sum - high - mid
        stats = jnp.where(sub == 0, high, jnp.where(sub == 1, mid, jnp.where(sub == 2, low, 0.0)))
        out_ref[pair, half : half + STAT_ROWS, :] = stats.astype(BF16)

    def rows_of(b):
        return slice(b * LANES, (b + 1) * LANES)

    def score(g, count, clear, s_ref, m_ref):
        none = jnp.zeros((half, LANES), BF16)
        q0, q1 = q_ref[2 * g], q_ref[2 * g + 1]
        placed = jnp.concatenate(
            [
                jnp.concatenate([jnp.where(left, q0, none), none], axis=1),
                jnp.concatenate([jnp.where(left, none, q0), none], axis=1),
                jnp.concatenate([none, jnp.where(left, q1, none)], axis=1),
                jnp.concatenate([none, jnp.where(left, none, q1)], axis=1),
            ],
            axis=0,
        )
        peak = None
        for b in range(count):
            part = jnp.dot(k_buf[g, rows_of(b), :], placed, preferred_element_type=F32)
            part = part * ks_ref[b : b + 1, lanes_of(g)]
            if b >= clear:
                place = b * LANES + lax.broadcasted_iota(jnp.int32, part.shape, 0)
                part = jnp.where(place < used, part, EMPTY)
            s_ref[rows_of(b), :] = part
            top = jnp.max(part, axis=0, keepdims=True)
            peak = top if peak is None else jnp.maximum(peak, top)
            yield
        m_ref[...] = peak

    def weigh(g, count, s_ref, m_ref, p_ref, n_ref):
        peak = m_ref[...]
        n_ref[...] = peak
        for b in range(count):
            shift = peak - lvs_ref[b : b + 1, lanes_of(g)]
            p_ref[rows_of(b), :] = jnp.exp2(s_ref[rows_of(b), :] - shift).astype(BF16)
            yield

    def gather(g, count, p_ref, n_ref):
        inverse_scale = ivs_ref[:, lanes_of(g)]
        for i in range(2):
            at = rows_of(i)
            sums = jnp.dot(
                vt_buf[g, i, :, 0 : count * LANES],
                p_ref[0 : count * LANES, at],
                preferred_element_type=F32,
            )
            yield
            total = jnp.sum(
                sums[LANES : LANES + count] * inverse_scale[0:count, at], axis=0, keepdims=True
            )
            mine = jnp.where(left, sums[0:half], sums[half:LANES])
            put(2 * g + i, mine * (1.0 / total), n_ref[:, at] + jnp.log2(total))
            yield

    def together(*stages):
        stages = list(stages)
        while stages:
            for stage in list(stages):
                if next(stage, stage) is stage:
                    stages.remove(stage)

    def run(count, clear):
        k_copy(0).wait()
        k_copy(1).wait()
        together(score(0, count, clear, s0, m0))
        together(score(1, count, clear, s1, m1), weigh(0, count, s0, m0, p0, n0))

        def two(i, carry):
            for g in (0, 1):
                k_copy(2 * i + g).wait()
                vt_copy(2 * i - 2 + g).wait()
            together(
                score(2 * i, count, clear, s0, m0),
                gather(2 * i - 2, count, p0, n0),
                weigh(2 * i - 1, count, s1, m1, p1, n1),
            )
            together(
                score(2 * i + 1, count, clear, s1, m1),
                gather(2 * i - 1, count, p1, n1),
                weigh(2 * i, count, s0, m0, p0, n0),
            )
            return carry

        lax.fori_loop(1, groups // 2, two, 0)
        vt_copy(groups - 2).wait()
        vt_copy(groups - 1).wait()
        together(gather(groups - 2, count, p0, n0), weigh(groups - 1, count, s1, m1, p1, n1))
        together(gather(groups - 1, count, p1, n1))

    most = (blocks - 1) * LANES

    @pl.when(used <= 0)
    def _():
        for g in range(groups):
            k_copy(g).wait()
            vt_copy(g).wait()
        for pair in range(2 * groups):
            put(pair, jnp.zeros((half, LANES), F32), jnp.full((1, LANES), EMPTY, F32))

    @pl.when((used > 0) & (used <= most))
    def _():
        run(blocks - 1, 0)

    @pl.when(used > most)
    def _():
        run(blocks, blocks - 1)


def output_kernel(rep_ref, part_ref, *refs):
    weights, out_ref = refs[:-1], refs[-1]
    segs = part_ref.shape[0]
    half = part_ref.shape[1] - STAT_ROWS
    log_sum = jnp.sum(part_ref[:, half : half + STAT_ROWS, :].astype(F32), axis=1)
    share = jnp.exp2(log_sum - jnp.max(log_sum, axis=0, keepdims=True))
    share = share / jnp.sum(share, axis=0, keepdims=True)
    total = jnp.zeros((half, LANES), F32)
    for j in range(segs):
        total += part_ref[j, 0:half, :].astype(F32) * share[j : j + 1, :]
    attended = flip_pair(total).astype(BF16)
    each = segs // len(weights)
    for i, w_ref in enumerate(weights):
        first = (rep_ref[0] ^ i) * each
        update = jnp.dot(attended, w_ref[...], preferred_element_type=F32)
        for j in range(each):
            out_ref[first + j] = update[:, j * LANES : (j + 1) * LANES].astype(BF16)


def sum_kernel(part_ref, out_ref):
    total = part_ref[0].astype(F32)
    for j in range(1, part_ref.shape[0]):
        total += part_ref[j].astype(F32)
    out_ref[...] = total.astype(BF16)


CORE = [(0, 1), (1, 0), (2, 3), (3, 2)]
CHIP = [(0, 2), (1, 3), (2, 0), (3, 1)]


def over_rep(block):
    far = lax.ppermute(block, "rep", CHIP)
    near = lax.ppermute(block, "rep", CORE)
    both = lax.ppermute(far, "rep", CORE)
    return block, near, far, both


def swapped(blocks):
    return lax.all_to_all(blocks, "seg", split_axis=0, concat_axis=0, tiled=True)


def sublayer(
    decoder_rows,
    norm_gain,
    query_weight,
    key_codes,
    key_scale,
    value_codes,
    value_scale,
    enc_lengths,
    output_weight,
):
    segs = lax.axis_size("seg")
    rows, own = decoder_rows.shape
    _, tokens, inner = key_codes.shape
    _, heads = key_scale.shape[1:]
    head_dim = inner // heads
    rep = lax.axis_index("rep").astype(jnp.int32).reshape(1)
    used = jnp.clip(enc_lengths - lax.axis_index("seg") * tokens, 0, tokens).astype(jnp.int32)
    gain = norm_gain.reshape(segs, own)
    key_lanes = jnp.repeat(key_scale[0] * LOG2E, head_dim, axis=1)
    value_logs = jnp.repeat(jnp.log2(value_scale[0]), head_dim, axis=1)
    value_inverse = jnp.repeat(1.0 / value_scale[0], head_dim, axis=1)

    wq, wq_near, wq_far, wq_both = over_rep(query_weight)
    x_all = swapped(jnp.broadcast_to(decoder_rows[None], (segs, rows, own)))
    wq, gain = pl.pallas_call(
        stage_kernel,
        out_shape=(
            jax.ShapeDtypeStruct(wq.shape, BF16),
            jax.ShapeDtypeStruct(gain.shape, F32),
        ),
        in_specs=[VMEM] * 2,
        out_specs=(VMEM, VMEM),
        compiler_params=params(8),
        cost_estimate=cost(1 << 24, 1 << 20),
        name="stage",
    )(wq, gain)
    query_call = pl.pallas_call(
        query_kernel,
        out_shape=jax.ShapeDtypeStruct((segs, head_dim, LANES), BF16),
        in_specs=[SMEM] + [VMEM] * 6,
        out_specs=VMEM,
        compiler_params=params(16),
        cost_estimate=cost(2 * rows * inner * own, 2 << 20),
        name="query",
    )
    query_sent = query_call(rep, x_all, gain, wq, wq_near, wq_far, wq_both)
    queries = swapped(query_sent)

    groups, wide = inner // (2 * LANES), 2 * LANES
    height = LANES + SUM_ROWS
    values_t = pl.pallas_call(
        turn_kernel,
        grid=(groups,),
        out_shape=jax.ShapeDtypeStruct((groups, 2, height, tokens), BF16),
        in_specs=[pl.BlockSpec((tokens, wide), lambda i: (0, i))],
        out_specs=pl.BlockSpec((1, 2, height, tokens), lambda i: (i, 0, 0, 0)),
        compiler_params=params(16),
        cost_estimate=cost(2 * inner * tokens * 512, 8 << 20),
        name="turn",
    )(value_codes[0])

    parts = pl.pallas_call(
        attend_kernel,
        out_shape=jax.ShapeDtypeStruct((segs, head_dim + STAT_ROWS, LANES), BF16),
        in_specs=[SMEM] + [VMEM] * 4 + [HBM] * 2,
        out_specs=VMEM,
        scratch_shapes=[
            pltpu.VMEM((groups, tokens, wide), BF16),
            pltpu.VMEM((groups, 2, height, tokens), BF16),
        ]
        + [pltpu.VMEM((tokens, wide), F32)] * 2
        + [pltpu.VMEM((tokens, wide), BF16)] * 2
        + [pltpu.VMEM((1, wide), F32)] * 4
        + [pltpu.SemaphoreType.DMA((groups,))] * 2,
        compiler_params=params(51),
        cost_estimate=cost(16 * rows * inner * tokens, 9 << 20),
        name="attend",
    )(used, queries, key_lanes, value_logs, value_inverse, key_codes[0], values_t)
    parts = swapped(parts)

    output_blocks = over_rep(output_weight)
    sent = pl.pallas_call(
        output_kernel,
        out_shape=jax.ShapeDtypeStruct((segs, rows, own), BF16),
        in_specs=[SMEM] + [VMEM] * 5,
        out_specs=VMEM,
        compiler_params=params(16),
        cost_estimate=cost(2 * rows * inner * own, 2 << 20),
        name="output",
    )(rep, parts, *output_blocks)
    return pl.pallas_call(
        sum_kernel,
        out_shape=jax.ShapeDtypeStruct((rows, own), BF16),
        in_specs=[VMEM],
        out_specs=VMEM,
        compiler_params=params(8),
        name="gather_sum",
    )(swapped(sent))


def solution(mesh):
    placed = (
        P("rep", "seg"),
        P(),
        P("rep", "seg"),
        P("rep", "seg", None),
        P("rep", "seg", None),
        P("rep", "seg", None),
        P("rep", "seg", None),
        P("rep"),
        P("seg", "rep"),
    )
    return jax.shard_map(
        sublayer, mesh=mesh, in_specs=placed, out_specs=P("rep", "seg"), check_vma=False
    )
```

```python
import math

import jax
import jax.numpy as jnp
from jax import lax
from jax.experimental import pallas as pl
from jax.experimental.pallas import tpu as pltpu
from jax.sharding import PartitionSpec as P

LOG2E = math.log2(math.e)
BF16, F32 = jnp.bfloat16, jnp.float32
LANES = 128
STAT_ROWS = 8
SUM_ROWS = 16
EMPTY = -1e30
FIRST = 10
VMEM = pl.BlockSpec(memory_space=pltpu.VMEM)
SMEM = pl.BlockSpec(memory_space=pltpu.SMEM)
HBM = pl.BlockSpec(memory_space=pltpu.HBM)


def params(mib):
    return pltpu.CompilerParams(vmem_limit_bytes=mib << 20)


def cost(flops, moved):
    return pl.CostEstimate(flops=flops, bytes_accessed=moved, transcendentals=0)


def flip_pair(block):
    half = block.shape[0]
    turned = jnp.concatenate([block, block], axis=0).T
    left = lax.broadcasted_iota(jnp.int32, block.shape, 1) < half
    return jnp.where(left, turned[:half], turned[half:])


def query_kernel(rep_ref, x_ref, gain_ref, *refs):
    weights, out_ref = refs[:-1], refs[-1]
    segs, rows, _ = x_ref.shape
    squares = jnp.zeros((rows, LANES), F32)
    for j in range(segs):
        wide = x_ref[j].astype(F32)
        squares += wide * wide
    mean = jnp.sum(squares, axis=1, keepdims=True) * (1.0 / (segs * LANES))
    scale = lax.rsqrt(mean + 1e-06)
    each = segs // len(weights)
    total = jnp.zeros((rows, LANES), F32)
    for i, w_ref in enumerate(weights):
        first = (rep_ref[0] ^ i) * each
        for j in range(0, each, 2):
            pair = [
                (x_ref[(first + k) ^ FIRST].astype(F32) * scale * gain_ref[pl.ds(first + k, 1), :]).astype(BF16)
                for k in (j, j + 1)
            ]
            total += jnp.dot(
                jnp.concatenate(pair, axis=1),
                w_ref[j * LANES : (j + 2) * LANES, :],
                preferred_element_type=F32,
            )
    own = flip_pair(total).astype(BF16)
    for j in range(segs):
        out_ref[j] = own


def stage_kernel(own_ref, gain_ref, own_out, gain_out):
    own_out[...] = own_ref[...]
    gain_out[...] = gain_ref[...]


def turn_kernel(v_ref, out_ref):
    tokens = v_ref.shape[0]
    row = lax.broadcasted_iota(jnp.int32, (SUM_ROWS, tokens), 0)
    block = lax.broadcasted_iota(jnp.int32, (SUM_ROWS, tokens), 1) // LANES
    picks = jnp.where(row == block, 1.0, 0.0).astype(BF16)
    for j in range(out_ref.shape[0]):
        for i in range(2):
            at = slice((2 * j + i) * LANES, (2 * j + i + 1) * LANES)
            out_ref[j, i, 0:LANES, :] = v_ref[:, at].T
            out_ref[j, i, LANES : LANES + SUM_ROWS, :] = picks


def attend_kernel(
    used_ref, q_ref, ks_ref, lvs_ref, ivs_ref, k_hbm, vt_hbm, out_ref,
    k_buf, vt_buf, s0, s1, p0, p1, m0, m1, n0, n1, k_sems, vt_sems,
):
    groups = vt_hbm.shape[0]
    half = q_ref.shape[1]
    blocks = ks_ref.shape[0]
    wide = 2 * LANES
    used = used_ref[0]
    sub = lax.broadcasted_iota(jnp.int32, (STAT_ROWS, LANES), 0)
    left = lax.broadcasted_iota(jnp.int32, (half, LANES), 1) < half

    def lanes_of(g):
        return pl.ds(g * wide if isinstance(g, int) else pl.multiple_of(g * wide, wide), wide)

    def k_copy(g):
        return pltpu.make_async_copy(k_hbm.at[:, lanes_of(g)], k_buf.at[g], k_sems.at[g])

    def vt_copy(g):
        return pltpu.make_async_copy(vt_hbm.at[g], vt_buf.at[g], vt_sems.at[g])

    for g in range(groups):
        k_copy(g).start()
        vt_copy(g).start()

    def put(pair, sums, log_sum):
        out_ref[pair ^ FIRST, 0:half, :] = sums.astype(BF16)
        high = log_sum.astype(BF16).astype(F32)
        mid = (log_sum - high).astype(BF16).astype(F32)
        low = log_sum - high - mid
        stats = jnp.where(sub == 0, high, jnp.where(sub == 1, mid, jnp.where(sub == 2, low, 0.0)))
        out_ref[pair ^ FIRST, half : half + STAT_ROWS, :] = stats.astype(BF16)

    def rows_of(b):
        return slice(b * LANES, (b + 1) * LANES)

    def score(g, count, clear, s_ref, m_ref):
        none = jnp.zeros((half, LANES), BF16)
        q0, q1 = q_ref[(2 * g) ^ FIRST], q_ref[(2 * g + 1) ^ FIRST]
        placed = jnp.concatenate(
            [
                jnp.concatenate([jnp.where(left, q0, none), none], axis=1),
                jnp.concatenate([jnp.where(left, none, q0), none], axis=1),
                jnp.concatenate([none, jnp.where(left, q1, none)], axis=1),
                jnp.concatenate([none, jnp.where(left, none, q1)], axis=1),
            ],
            axis=0,
        )
        peak = None
        for b in range(count):
            part = jnp.dot(k_buf[g, rows_of(b), :], placed, preferred_element_type=F32)
            part = part * ks_ref[b : b + 1, lanes_of(g)]
            if b >= clear:
                place = b * LANES + lax.broadcasted_iota(jnp.int32, part.shape, 0)
                part = jnp.where(place < used, part, EMPTY)
            s_ref[rows_of(b), :] = part
            top = jnp.max(part, axis=0, keepdims=True)
            peak = top if peak is None else jnp.maximum(peak, top)
            yield
        m_ref[...] = peak

    def weigh(g, count, s_ref, m_ref, p_ref, n_ref):
        peak = m_ref[...]
        n_ref[...] = peak
        for b in range(count):
            shift = peak - lvs_ref[b : b + 1, lanes_of(g)]
            p_ref[rows_of(b), :] = jnp.exp2(s_ref[rows_of(b), :] - shift).astype(BF16)
            yield

    def gather(g, count, p_ref, n_ref):
        inverse_scale = ivs_ref[:, lanes_of(g)]
        for i in range(2):
            at = rows_of(i)
            sums = jnp.dot(
                vt_buf[g, i, :, 0 : count * LANES],
                p_ref[0 : count * LANES, at],
                preferred_element_type=F32,
            )
            yield
            total = jnp.sum(
                sums[LANES : LANES + count] * inverse_scale[0:count, at], axis=0, keepdims=True
            )
            mine = jnp.where(left, sums[0:half], sums[half:LANES])
            put(2 * g + i, mine * (1.0 / total), n_ref[:, at] + jnp.log2(total))
            yield

    def together(*stages):
        stages = list(stages)
        while stages:
            for stage in list(stages):
                if next(stage, stage) is stage:
                    stages.remove(stage)

    def run(count, clear):
        k_copy(0).wait()
        k_copy(1).wait()
        together(score(0, count, clear, s0, m0))
        together(score(1, count, clear, s1, m1), weigh(0, count, s0, m0, p0, n0))

        def two(i, carry):
            for g in (0, 1):
                k_copy(2 * i + g).wait()
                vt_copy(2 * i - 2 + g).wait()
            together(
                score(2 * i, count, clear, s0, m0),
                gather(2 * i - 2, count, p0, n0),
                weigh(2 * i - 1, count, s1, m1, p1, n1),
            )
            together(
                score(2 * i + 1, count, clear, s1, m1),
                gather(2 * i - 1, count, p1, n1),
                weigh(2 * i, count, s0, m0, p0, n0),
            )
            return carry

        lax.fori_loop(1, groups // 2, two, 0)
        vt_copy(groups - 2).wait()
        vt_copy(groups - 1).wait()
        together(gather(groups - 2, count, p0, n0), weigh(groups - 1, count, s1, m1, p1, n1))
        together(gather(groups - 1, count, p1, n1))

    most = (blocks - 1) * LANES

    @pl.when(used <= 0)
    def _():
        for g in range(groups):
            k_copy(g).wait()
            vt_copy(g).wait()
        for pair in range(2 * groups):
            put(pair, jnp.zeros((half, LANES), F32), jnp.full((1, LANES), EMPTY, F32))

    @pl.when((used > 0) & (used <= most))
    def _():
        run(blocks - 1, 0)

    @pl.when(used > most)
    def _():
        run(blocks, blocks - 1)


def output_kernel(rep_ref, part_ref, *refs):
    weights, out_ref = refs[:-1], refs[-1]
    segs = part_ref.shape[0]
    half = part_ref.shape[1] - STAT_ROWS
    log_sum = jnp.sum(part_ref[:, half : half + STAT_ROWS, :].astype(F32), axis=1)
    share = jnp.exp2(log_sum - jnp.max(log_sum, axis=0, keepdims=True))
    share = share / jnp.sum(share, axis=0, keepdims=True)
    total = jnp.zeros((half, LANES), F32)
    for j in range(segs):
        total += part_ref[j, 0:half, :].astype(F32) * share[j : j + 1, :]
    attended = flip_pair(total).astype(BF16)
    each = segs // len(weights)
    for i, w_ref in enumerate(weights):
        first = (rep_ref[0] ^ i) * each
        update = jnp.dot(attended, w_ref[...], preferred_element_type=F32)
        for j in range(each):
            out_ref[(first + j) ^ FIRST] = update[:, j * LANES : (j + 1) * LANES].astype(BF16)


def sum_kernel(part_ref, out_ref):
    total = part_ref[0].astype(F32)
    for j in range(1, part_ref.shape[0]):
        total += part_ref[j].astype(F32)
    out_ref[...] = total.astype(BF16)


CORE = [(0, 1), (1, 0), (2, 3), (3, 2)]
CHIP = [(0, 2), (1, 3), (2, 0), (3, 1)]


def over_rep(block):
    far = lax.ppermute(block, "rep", CHIP)
    near = lax.ppermute(block, "rep", CORE)
    both = lax.ppermute(far, "rep", CORE)
    return block, near, far, both


def swapped(blocks):
    order = [[j ^ FIRST for j in range(blocks.shape[0])]]
    return lax.all_to_all(
        blocks, "seg", split_axis=0, concat_axis=0, tiled=True, axis_index_groups=order
    )


def sublayer(
    decoder_rows,
    norm_gain,
    query_weight,
    key_codes,
    key_scale,
    value_codes,
    value_scale,
    enc_lengths,
    output_weight,
):
    segs = lax.axis_size("seg")
    rows, own = decoder_rows.shape
    _, tokens, inner = key_codes.shape
    _, heads = key_scale.shape[1:]
    head_dim = inner // heads
    rep = lax.axis_index("rep").astype(jnp.int32).reshape(1)
    used = jnp.clip(enc_lengths - lax.axis_index("seg") * tokens, 0, tokens).astype(jnp.int32)
    gain = norm_gain.reshape(segs, own)
    key_lanes = jnp.repeat(key_scale[0] * LOG2E, head_dim, axis=1)
    value_logs = jnp.repeat(jnp.log2(value_scale[0]), head_dim, axis=1)
    value_inverse = jnp.repeat(1.0 / value_scale[0], head_dim, axis=1)

    wq, wq_near, wq_far, wq_both = over_rep(query_weight)
    x_all = swapped(jnp.broadcast_to(decoder_rows[None], (segs, rows, own)))
    groups, wide = inner // (2 * LANES), 2 * LANES
    height = LANES + SUM_ROWS
    steps = 4
    turn_call = pl.pallas_call(
        turn_kernel,
        grid=(steps,),
        out_shape=jax.ShapeDtypeStruct((groups, 2, height, tokens), BF16),
        in_specs=[pl.BlockSpec((tokens, inner // steps), lambda i: (0, i))],
        out_specs=pl.BlockSpec((groups // steps, 2, height, tokens), lambda i: (i, 0, 0, 0)),
        compiler_params=params(51),
        cost_estimate=cost(2 * inner * tokens * 512, 8 << 20),
        name="turn",
    )
    values_t = turn_call(value_codes[0])

    stage_call = pl.pallas_call(
        stage_kernel,
        out_shape=(
            jax.ShapeDtypeStruct(wq.shape, BF16),
            jax.ShapeDtypeStruct(gain.shape, F32),
        ),
        in_specs=[VMEM] * 2,
        out_specs=(VMEM, VMEM),
        compiler_params=params(8),
        cost_estimate=cost(1 << 24, 1 << 20),
        name="stage",
    )
    wq, gain = stage_call(wq, gain)
    query_call = pl.pallas_call(
        query_kernel,
        out_shape=jax.ShapeDtypeStruct((segs, head_dim, LANES), BF16),
        in_specs=[SMEM] + [VMEM] * 6,
        out_specs=VMEM,
        compiler_params=params(16),
        cost_estimate=cost(2 * rows * inner * own, 2 << 20),
        name="query",
    )
    query_sent = query_call(rep, x_all, gain, wq, wq_near, wq_far, wq_both)
    queries = swapped(query_sent)

    parts = pl.pallas_call(
        attend_kernel,
        out_shape=jax.ShapeDtypeStruct((segs, head_dim + STAT_ROWS, LANES), BF16),
        in_specs=[SMEM] + [VMEM] * 4 + [HBM] * 2,
        out_specs=VMEM,
        scratch_shapes=[
            pltpu.VMEM((groups, tokens, wide), BF16),
            pltpu.VMEM((groups, 2, height, tokens), BF16),
        ]
        + [pltpu.VMEM((tokens, wide), F32)] * 2
        + [pltpu.VMEM((tokens, wide), BF16)] * 2
        + [pltpu.VMEM((1, wide), F32)] * 4
        + [pltpu.SemaphoreType.DMA((groups,))] * 2,
        compiler_params=params(51),
        cost_estimate=cost(16 * rows * inner * tokens, 9 << 20),
        name="attend",
    )(used, queries, key_lanes, value_logs, value_inverse, key_codes[0], values_t)
    parts = swapped(parts)

    output_blocks = over_rep(output_weight)
    sent = pl.pallas_call(
        output_kernel,
        out_shape=jax.ShapeDtypeStruct((segs, rows, own), BF16),
        in_specs=[SMEM] + [VMEM] * 5,
        out_specs=VMEM,
        compiler_params=params(16),
        cost_estimate=cost(2 * rows * inner * own, 2 << 20),
        name="output",
    )(rep, parts, *output_blocks)
    return pl.pallas_call(
        sum_kernel,
        out_shape=jax.ShapeDtypeStruct((rows, own), BF16),
        in_specs=[VMEM],
        out_specs=VMEM,
        compiler_params=params(8),
        name="gather_sum",
    )(swapped(sent))


def solution(mesh):
    placed = (
        P("rep", "seg"),
        P(),
        P("rep", "seg"),
        P("rep", "seg", None),
        P("rep", "seg", None),
        P("rep", "seg", None),
        P("rep", "seg", None),
        P("rep"),
        P("seg", "rep"),
    )
    return jax.shard_map(
        sublayer, mesh=mesh, in_specs=placed, out_specs=P("rep", "seg"), check_vma=False
    )
```

```python
import math

import jax
import jax.numpy as jnp
from jax import lax
from jax.experimental import pallas as pl
from jax.experimental.pallas import tpu as pltpu
from jax.sharding import PartitionSpec as P

LOG2E = math.log2(math.e)
BF16, F32 = jnp.bfloat16, jnp.float32
LANES = 128
STAT_ROWS = 8
SUM_ROWS = 16
EMPTY = -1e30
FIRST = 10
LAST = 26
VMEM = pl.BlockSpec(memory_space=pltpu.VMEM)
SMEM = pl.BlockSpec(memory_space=pltpu.SMEM)
HBM = pl.BlockSpec(memory_space=pltpu.HBM)


def params(mib):
    return pltpu.CompilerParams(vmem_limit_bytes=mib << 20)


def cost(flops, moved):
    return pl.CostEstimate(flops=flops, bytes_accessed=moved, transcendentals=0)


def flip_pair(block):
    half = block.shape[0]
    turned = jnp.concatenate([block, block], axis=0).T
    left = lax.broadcasted_iota(jnp.int32, block.shape, 1) < half
    return jnp.where(left, turned[:half], turned[half:])


def query_kernel(rep_ref, x_ref, gain_ref, *refs):
    weights, out_ref = refs[:-1], refs[-1]
    segs, rows, _ = x_ref.shape
    squares = jnp.zeros((rows, LANES), F32)
    for j in range(segs):
        wide = x_ref[j].astype(F32)
        squares += wide * wide
    mean = jnp.sum(squares, axis=1, keepdims=True) * (1.0 / (segs * LANES))
    scale = lax.rsqrt(mean + 1e-06)
    each = segs // len(weights)
    total = jnp.zeros((rows, LANES), F32)
    for i, w_ref in enumerate(weights):
        first = (rep_ref[0] ^ i) * each
        for j in range(0, each, 2):
            pair = [
                (x_ref[(first + k) ^ FIRST].astype(F32) * scale * gain_ref[pl.ds(first + k, 1), :]).astype(BF16)
                for k in (j, j + 1)
            ]
            total += jnp.dot(
                jnp.concatenate(pair, axis=1),
                w_ref[j * LANES : (j + 2) * LANES, :],
                preferred_element_type=F32,
            )
    own = flip_pair(total).astype(BF16)
    for j in range(segs):
        out_ref[j] = own


def stage_kernel(own_ref, gain_ref, own_out, gain_out):
    own_out[...] = own_ref[...]
    gain_out[...] = gain_ref[...]


def picks_of(tokens):
    row = lax.broadcasted_iota(jnp.int32, (SUM_ROWS, tokens), 0)
    block = lax.broadcasted_iota(jnp.int32, (SUM_ROWS, tokens), 1) // LANES
    return jnp.where(row == block, 1.0, 0.0).astype(BF16)


def turn_kernel(v_ref, k_ref, out_ref, k_first, vt_first):
    for j in range(out_ref.shape[0]):
        for i in range(2):
            at = slice((2 * j + i) * LANES, (2 * j + i + 1) * LANES)
            out_ref[j, i] = v_ref[:, at].T

    @pl.when(pl.program_id(0) == 0)
    def _():
        for g in range(k_first.shape[0]):
            k_first[g] = k_ref[:, 2 * g * LANES : 2 * (g + 1) * LANES]
        picks = picks_of(v_ref.shape[0])
        for j in range(vt_first.shape[0]):
            for i in range(2):
                vt_first[j, i, 0:LANES, :] = out_ref[j, i]
                vt_first[j, i, LANES : LANES + SUM_ROWS, :] = picks


def attend_kernel(
    used_ref, q_ref, ks_ref, lvs_ref, ivs_ref, k_first, vt_first, k_hbm, vt_hbm, out_hbm,
    out_ref, k_buf, vt_buf, s0, s1, p0, p1, m0, m1, n0, n1, k_sems, vt_sems, out_sems,
):
    groups = vt_hbm.shape[0]
    half = q_ref.shape[1]
    blocks = ks_ref.shape[0]
    wide = 2 * LANES
    used = used_ref[0]
    sub = lax.broadcasted_iota(jnp.int32, (STAT_ROWS, LANES), 0)
    left = lax.broadcasted_iota(jnp.int32, (half, LANES), 1) < half

    def lanes_of(g):
        return pl.ds(g * wide if isinstance(g, int) else pl.multiple_of(g * wide, wide), wide)

    def k_copy(g):
        return pltpu.make_async_copy(k_hbm.at[:, lanes_of(g)], k_buf.at[g], k_sems.at[g])

    def vt_copy(g):
        return pltpu.make_async_copy(
            vt_hbm.at[g], vt_buf.at[g, :, pl.ds(0, LANES), :], vt_sems.at[g]
        )

    def out_copy(g):
        at = pl.ds((2 * g) ^ FIRST, 2)
        return pltpu.make_async_copy(out_ref.at[at], out_hbm.at[at], out_sems.at[g])

    k_early, vt_early = k_first.shape[0], vt_first.shape[0]

    def fetch(i):
        for g in (2 * i, 2 * i + 1):
            if not isinstance(i, int) or g < groups:
                k_copy(g).start()
            vt_copy(g - 2).start()

    for i in range(2, groups // 2 + 1):
        fetch(i)

    picks = picks_of(k_buf.shape[1])
    for g in range(vt_early, groups):
        for i in range(2):
            vt_buf[g, i, LANES : LANES + SUM_ROWS, :] = picks

    def put(pair, sums, log_sum):
        out_ref[pair ^ FIRST, 0:half, :] = sums.astype(BF16)
        high = log_sum.astype(BF16).astype(F32)
        mid = (log_sum - high).astype(BF16).astype(F32)
        low = log_sum - high - mid
        stats = jnp.where(sub == 0, high, jnp.where(sub == 1, mid, jnp.where(sub == 2, low, 0.0)))
        out_ref[pair ^ FIRST, half : half + STAT_ROWS, :] = stats.astype(BF16)

    def rows_of(b):
        return slice(b * LANES, (b + 1) * LANES)

    def score(g, count, clear, s_ref, m_ref):
        none = jnp.zeros((half, LANES), BF16)
        q0, q1 = q_ref[(2 * g) ^ FIRST], q_ref[(2 * g + 1) ^ FIRST]
        placed = jnp.concatenate(
            [
                jnp.concatenate([jnp.where(left, q0, none), none], axis=1),
                jnp.concatenate([jnp.where(left, none, q0), none], axis=1),
                jnp.concatenate([none, jnp.where(left, q1, none)], axis=1),
                jnp.concatenate([none, jnp.where(left, none, q1)], axis=1),
            ],
            axis=0,
        )
        peak = None
        keys = k_first if isinstance(g, int) and g < k_early else k_buf
        for b in range(count):
            part = jnp.dot(keys[g, rows_of(b), :], placed, preferred_element_type=F32)
            part = part * ks_ref[b : b + 1, lanes_of(g)]
            if b >= clear:
                place = b * LANES + lax.broadcasted_iota(jnp.int32, part.shape, 0)
                part = jnp.where(place < used, part, EMPTY)
            s_ref[rows_of(b), :] = part
            top = jnp.max(part, axis=0, keepdims=True)
            peak = top if peak is None else jnp.maximum(peak, top)
            yield
        m_ref[...] = peak

    def weigh(g, count, s_ref, m_ref, p_ref, n_ref):
        peak = m_ref[...]
        n_ref[...] = peak
        for b in range(count):
            shift = peak - lvs_ref[b : b + 1, lanes_of(g)]
            p_ref[rows_of(b), :] = jnp.exp2(s_ref[rows_of(b), :] - shift).astype(BF16)
            yield

    def gather(g, count, p_ref, n_ref):
        inverse_scale = ivs_ref[:, lanes_of(g)]
        for i in range(2):
            at = rows_of(i)
            values = vt_first if isinstance(g, int) and g < vt_early else vt_buf
            sums = jnp.dot(
                values[g, i, :, 0 : count * LANES],
                p_ref[0 : count * LANES, at],
                preferred_element_type=F32,
            )
            yield
            total = jnp.sum(
                sums[LANES : LANES + count] * inverse_scale[0:count, at], axis=0, keepdims=True
            )
            mine = jnp.where(left, sums[0:half], sums[half:LANES])
            put(2 * g + i, mine * (1.0 / total), n_ref[:, at] + jnp.log2(total))
            yield

    def together(*stages):
        stages = list(stages)
        while stages:
            for stage in list(stages):
                if next(stage, stage) is stage:
                    stages.remove(stage)

    def run(count, clear):
        together(score(0, count, clear, s0, m0))
        together(score(1, count, clear, s1, m1), weigh(0, count, s0, m0, p0, n0))

        def two(i):
            together(
                gather(2 * i - 2, count, p0, n0),
                score(2 * i, count, clear, s0, m0),
                weigh(2 * i - 1, count, s1, m1, p1, n1),
            )
            together(
                gather(2 * i - 1, count, p1, n1),
                score(2 * i + 1, count, clear, s1, m1),
                weigh(2 * i, count, s0, m0, p0, n0),
            )

        def more(i, carry):
            for g in (2 * i, 2 * i + 1):
                k_copy(g).wait()
                vt_copy(g - 2).wait()
                out_copy(g - 4).start()

            two(i)
            return carry

        steps = groups // 2
        two(1)
        lax.fori_loop(2, steps, more, 0)
        out_copy(groups - 4).start()
        out_copy(groups - 3).start()
        vt_copy(groups - 2).wait()
        vt_copy(groups - 1).wait()
        together(gather(groups - 2, count, p0, n0), weigh(groups - 1, count, s1, m1, p1, n1))
        out_copy(groups - 2).start()
        together(gather(groups - 1, count, p1, n1))
        out_copy(groups - 1).start()
        for g in range(groups):
            out_copy(g).wait()

    most = (blocks - 1) * LANES

    @pl.when(used <= 0)
    def _():
        for pair in range(2 * groups):
            put(pair, jnp.zeros((half, LANES), F32), jnp.full((1, LANES), EMPTY, F32))
        for g in range(groups):
            out_copy(g).start()
        for g in range(4, groups + 2):
            if g < groups:
                k_copy(g).wait()
            vt_copy(g - 2).wait()
        for g in range(groups):
            out_copy(g).wait()

    @pl.when((used > 0) & (used <= most))
    def _():
        run(blocks - 1, 0)

    @pl.when(used > most)
    def _():
        run(blocks, blocks - 1)


def output_kernel(rep_ref, part_ref, *refs):
    weights, out_ref = refs[:-1], refs[-1]
    segs = part_ref.shape[0]
    half = part_ref.shape[1] - STAT_ROWS
    log_sum = jnp.sum(part_ref[:, half : half + STAT_ROWS, :].astype(F32), axis=1)
    share = jnp.exp2(log_sum - jnp.max(log_sum, axis=0, keepdims=True))
    share = share / jnp.sum(share, axis=0, keepdims=True)
    total = jnp.zeros((half, LANES), F32)
    for j in range(segs):
        total += part_ref[j, 0:half, :].astype(F32) * share[j : j + 1, :]
    attended = flip_pair(total).astype(BF16)
    each = segs // len(weights)
    for i, w_ref in enumerate(weights):
        first = (rep_ref[0] ^ i) * each
        update = jnp.dot(attended, w_ref[...], preferred_element_type=F32)
        for j in range(each):
            out_ref[(first + j) ^ LAST] = update[:, j * LANES : (j + 1) * LANES].astype(BF16)


def sum_kernel(part_ref, out_ref):
    total = part_ref[0].astype(F32)
    for j in range(1, part_ref.shape[0]):
        total += part_ref[j].astype(F32)
    out_ref[...] = total.astype(BF16)


CORE = [(0, 1), (1, 0), (2, 3), (3, 2)]
CHIP = [(0, 2), (1, 3), (2, 0), (3, 1)]


def over_rep(block):
    far = lax.ppermute(block, "rep", CHIP)
    near = lax.ppermute(block, "rep", CORE)
    both = lax.ppermute(far, "rep", CORE)
    return block, near, far, both


def swapped(blocks, lead=FIRST):
    order = [[j ^ lead for j in range(blocks.shape[0])]]
    return lax.all_to_all(
        blocks, "seg", split_axis=0, concat_axis=0, tiled=True, axis_index_groups=order
    )


def sublayer(
    decoder_rows,
    norm_gain,
    query_weight,
    key_codes,
    key_scale,
    value_codes,
    value_scale,
    enc_lengths,
    output_weight,
):
    segs = lax.axis_size("seg")
    rows, own = decoder_rows.shape
    _, tokens, inner = key_codes.shape
    _, heads = key_scale.shape[1:]
    head_dim = inner // heads
    rep = lax.axis_index("rep").astype(jnp.int32).reshape(1)
    used = jnp.clip(enc_lengths - lax.axis_index("seg") * tokens, 0, tokens).astype(jnp.int32)
    gain = norm_gain.reshape(segs, own)
    key_lanes = jnp.repeat(key_scale[0] * LOG2E, head_dim, axis=1)
    value_logs = jnp.repeat(jnp.log2(value_scale[0]), head_dim, axis=1)
    value_inverse = jnp.repeat(1.0 / value_scale[0], head_dim, axis=1)

    wq, wq_near, wq_far, wq_both = over_rep(query_weight)
    x_all = swapped(jnp.broadcast_to(decoder_rows[None], (segs, rows, own)))
    groups, wide = inner // (2 * LANES), 2 * LANES
    height = LANES + SUM_ROWS
    steps = 4
    turn_call = pl.pallas_call(
        turn_kernel,
        grid=(steps,),
        out_shape=(
            jax.ShapeDtypeStruct((groups, 2, LANES, tokens), BF16),
            jax.ShapeDtypeStruct((4, tokens, wide), BF16),
            jax.ShapeDtypeStruct((2, 2, height, tokens), BF16),
        ),
        in_specs=[
            pl.BlockSpec((tokens, inner // steps), lambda i: (0, i)),
            pl.BlockSpec((tokens, 4 * wide), lambda i: (0, 0)),
        ],
        out_specs=(
            pl.BlockSpec((groups // steps, 2, LANES, tokens), lambda i: (i, 0, 0, 0)),
            pl.BlockSpec((4, tokens, wide), lambda i: (0, 0, 0)),
            pl.BlockSpec((2, 2, height, tokens), lambda i: (0, 0, 0, 0)),
        ),
        compiler_params=params(51),
        cost_estimate=cost(2 * inner * tokens * 512, 8 << 20),
        name="turn",
    )
    values_t, first_keys, first_values = turn_call(value_codes[0], key_codes[0])

    stage_call = pl.pallas_call(
        stage_kernel,
        out_shape=(
            jax.ShapeDtypeStruct(wq.shape, BF16),
            jax.ShapeDtypeStruct(gain.shape, F32),
        ),
        in_specs=[VMEM] * 2,
        out_specs=(VMEM, VMEM),
        compiler_params=params(8),
        cost_estimate=cost(1 << 24, 1 << 20),
        name="stage",
    )
    wq, gain = stage_call(wq, gain)
    query_call = pl.pallas_call(
        query_kernel,
        out_shape=jax.ShapeDtypeStruct((segs, head_dim, LANES), BF16),
        in_specs=[SMEM] + [VMEM] * 6,
        out_specs=VMEM,
        compiler_params=params(16),
        cost_estimate=cost(2 * rows * inner * own, 2 << 20),
        name="query",
    )
    x_all, key_lanes, value_logs, value_inverse = lax.optimization_barrier(
        (x_all, key_lanes, value_logs, value_inverse)
    )
    query_sent = query_call(rep, x_all, gain, wq, wq_near, wq_far, wq_both)
    queries = swapped(query_sent)

    parts = pl.pallas_call(
        attend_kernel,
        out_shape=jax.ShapeDtypeStruct((segs, head_dim + STAT_ROWS, LANES), BF16),
        in_specs=[SMEM] + [VMEM] * 6 + [HBM] * 2,
        out_specs=HBM,
        scratch_shapes=[
            pltpu.VMEM((segs, head_dim + STAT_ROWS, LANES), BF16),
            pltpu.VMEM((groups, tokens, wide), BF16),
            pltpu.VMEM((groups, 2, height, tokens), BF16),
        ]
        + [pltpu.VMEM((tokens, wide), F32)] * 2
        + [pltpu.VMEM((tokens, wide), BF16)] * 2
        + [pltpu.VMEM((1, wide), F32)] * 4
        + [pltpu.SemaphoreType.DMA((groups,))] * 3,
        compiler_params=params(51),
        cost_estimate=cost(16 * rows * inner * tokens, 9 << 20),
        name="attend",
    )(used, queries, key_lanes, value_logs, value_inverse, first_keys, first_values, key_codes[0], values_t)
    parts = swapped(parts)

    output_blocks = over_rep(output_weight)
    sent = pl.pallas_call(
        output_kernel,
        out_shape=jax.ShapeDtypeStruct((segs, rows, own), BF16),
        in_specs=[SMEM] + [VMEM] * 5,
        out_specs=VMEM,
        compiler_params=params(16),
        cost_estimate=cost(2 * rows * inner * own, 2 << 20),
        name="output",
    )(rep, parts, *output_blocks)
    return pl.pallas_call(
        sum_kernel,
        out_shape=jax.ShapeDtypeStruct((rows, own), BF16),
        in_specs=[VMEM],
        out_specs=VMEM,
        compiler_params=params(8),
        name="gather_sum",
    )(swapped(sent, LAST))


def solution(mesh):
    placed = (
        P("rep", "seg"),
        P(),
        P("rep", "seg"),
        P("rep", "seg", None),
        P("rep", "seg", None),
        P("rep", "seg", None),
        P("rep", "seg", None),
        P("rep"),
        P("seg", "rep"),
    )
    return jax.shard_map(
        sublayer, mesh=mesh, in_specs=placed, out_specs=P("rep", "seg"), check_vma=False
    )
```

```python
import math

import jax
import jax.numpy as jnp
from jax import lax
from jax.experimental import pallas as pl
from jax.experimental.pallas import tpu as pltpu
from jax.sharding import PartitionSpec as P

LOG2E = math.log2(math.e)
BF16, F32 = jnp.bfloat16, jnp.float32
LANES = 128
STAT_ROWS = 8
SUM_ROWS = 16
EMPTY = -1e30
FIRST = 26
VMEM = pl.BlockSpec(memory_space=pltpu.VMEM)
SMEM = pl.BlockSpec(memory_space=pltpu.SMEM)
HBM = pl.BlockSpec(memory_space=pltpu.HBM)


def params(mib):
    return pltpu.CompilerParams(vmem_limit_bytes=mib << 20)


def cost(flops, moved):
    return pl.CostEstimate(flops=flops, bytes_accessed=moved, transcendentals=0)


def flip_pair(block):
    half = block.shape[0]
    turned = jnp.concatenate([block, block], axis=0).T
    left = lax.broadcasted_iota(jnp.int32, block.shape, 1) < half
    return jnp.where(left, turned[:half], turned[half:])


def query_kernel(rep_ref, x_ref, gain_ref, *refs):
    weights, out_ref = refs[:-1], refs[-1]
    segs, rows, _ = x_ref.shape
    squares = jnp.zeros((rows, LANES), F32)
    for j in range(segs):
        wide = x_ref[j].astype(F32)
        squares += wide * wide
    mean = jnp.sum(squares, axis=1, keepdims=True) * (1.0 / (segs * LANES))
    scale = lax.rsqrt(mean + 1e-06)
    each = segs // len(weights)
    total = jnp.zeros((rows, LANES), F32)
    for i, w_ref in enumerate(weights):
        first = (rep_ref[0] ^ i) * each
        for j in range(0, each, 2):
            pair = [
                (x_ref[(first + k) ^ FIRST].astype(F32) * scale * gain_ref[pl.ds(first + k, 1), :]).astype(BF16)
                for k in (j, j + 1)
            ]
            total += jnp.dot(
                jnp.concatenate(pair, axis=1),
                w_ref[j * LANES : (j + 2) * LANES, :],
                preferred_element_type=F32,
            )
    own = flip_pair(total).astype(BF16)
    for j in range(segs):
        out_ref[j] = own


def stage_kernel(own_ref, gain_ref, own_out, gain_out):
    own_out[...] = own_ref[...]
    gain_out[...] = gain_ref[...]


def turn_kernel(v_ref, k_ref, out_ref, k_first, vt_first):
    tokens = v_ref.shape[0]
    row = lax.broadcasted_iota(jnp.int32, (SUM_ROWS, tokens), 0)
    block = lax.broadcasted_iota(jnp.int32, (SUM_ROWS, tokens), 1) // LANES
    picks = jnp.where(row == block, 1.0, 0.0).astype(BF16)
    for j in range(out_ref.shape[0]):
        for i in range(2):
            at = slice((2 * j + i) * LANES, (2 * j + i + 1) * LANES)
            out_ref[j, i, 0:LANES, :] = v_ref[:, at].T
            out_ref[j, i, LANES : LANES + SUM_ROWS, :] = picks

    @pl.when(pl.program_id(0) == 0)
    def _():
        for g in range(k_first.shape[0]):
            k_first[g] = k_ref[:, 2 * g * LANES : 2 * (g + 1) * LANES]
        vt_first[...] = out_ref[0 : vt_first.shape[0]]


def attend_kernel(
    used_ref, q_ref, ks_ref, lvs_ref, ivs_ref, k_first, vt_first, k_hbm, vt_hbm, out_hbm,
    out_ref, k_buf, vt_buf, s0, s1, p0, p1, m0, m1, n0, n1, k_sems, vt_sems, out_sems,
):
    groups = vt_hbm.shape[0]
    half = q_ref.shape[1]
    blocks = ks_ref.shape[0]
    wide = 2 * LANES
    used = used_ref[0]
    sub = lax.broadcasted_iota(jnp.int32, (STAT_ROWS, LANES), 0)
    left = lax.broadcasted_iota(jnp.int32, (half, LANES), 1) < half

    def lanes_of(g):
        return pl.ds(g * wide if isinstance(g, int) else pl.multiple_of(g * wide, wide), wide)

    def k_copy(g):
        return pltpu.make_async_copy(k_hbm.at[:, lanes_of(g)], k_buf.at[g], k_sems.at[g])

    def vt_copy(g):
        return pltpu.make_async_copy(vt_hbm.at[g], vt_buf.at[g], vt_sems.at[g])

    def out_copy(g):
        at = pl.ds((2 * g) ^ FIRST, 2)
        return pltpu.make_async_copy(out_ref.at[at], out_hbm.at[at], out_sems.at[g])

    k_early, vt_early = k_first.shape[0], vt_first.shape[0]

    def fetch(i):
        for g in (2 * i, 2 * i + 1):
            if not isinstance(i, int) or g < groups:
                k_copy(g).start()
            vt_copy(g - 2).start()

    for i in range(2, groups // 2 + 1):
        fetch(i)

    def put(pair, sums, log_sum):
        out_ref[pair ^ FIRST, 0:half, :] = sums.astype(BF16)
        high = log_sum.astype(BF16).astype(F32)
        mid = (log_sum - high).astype(BF16).astype(F32)
        low = log_sum - high - mid
        stats = jnp.where(sub == 0, high, jnp.where(sub == 1, mid, jnp.where(sub == 2, low, 0.0)))
        out_ref[pair ^ FIRST, half : half + STAT_ROWS, :] = stats.astype(BF16)

    def rows_of(b):
        return slice(b * LANES, (b + 1) * LANES)

    def score(g, count, clear, s_ref, m_ref):
        none = jnp.zeros((half, LANES), BF16)
        q0, q1 = q_ref[(2 * g) ^ FIRST], q_ref[(2 * g + 1) ^ FIRST]
        placed = jnp.concatenate(
            [
                jnp.concatenate([jnp.where(left, q0, none), none], axis=1),
                jnp.concatenate([jnp.where(left, none, q0), none], axis=1),
                jnp.concatenate([none, jnp.where(left, q1, none)], axis=1),
                jnp.concatenate([none, jnp.where(left, none, q1)], axis=1),
            ],
            axis=0,
        )
        peak = None
        keys = k_first if isinstance(g, int) and g < k_early else k_buf
        for b in range(count):
            part = jnp.dot(keys[g, rows_of(b), :], placed, preferred_element_type=F32)
            part = part * ks_ref[b : b + 1, lanes_of(g)]
            if b >= clear:
                place = b * LANES + lax.broadcasted_iota(jnp.int32, part.shape, 0)
                part = jnp.where(place < used, part, EMPTY)
            s_ref[rows_of(b), :] = part
            top = jnp.max(part, axis=0, keepdims=True)
            peak = top if peak is None else jnp.maximum(peak, top)
            yield
        m_ref[...] = peak

    def weigh(g, count, s_ref, m_ref, p_ref, n_ref):
        peak = m_ref[...]
        n_ref[...] = peak
        for b in range(count):
            shift = peak - lvs_ref[b : b + 1, lanes_of(g)]
            p_ref[rows_of(b), :] = jnp.exp2(s_ref[rows_of(b), :] - shift).astype(BF16)
            yield

    def gather(g, count, p_ref, n_ref):
        inverse_scale = ivs_ref[:, lanes_of(g)]
        for i in range(2):
            at = rows_of(i)
            values = vt_first if isinstance(g, int) and g < vt_early else vt_buf
            sums = jnp.dot(
                values[g, i, :, 0 : count * LANES],
                p_ref[0 : count * LANES, at],
                preferred_element_type=F32,
            )
            yield
            total = jnp.sum(
                sums[LANES : LANES + count] * inverse_scale[0:count, at], axis=0, keepdims=True
            )
            mine = jnp.where(left, sums[0:half], sums[half:LANES])
            put(2 * g + i, mine * (1.0 / total), n_ref[:, at] + jnp.log2(total))
            yield

    def together(*stages):
        stages = list(stages)
        while stages:
            for stage in list(stages):
                if next(stage, stage) is stage:
                    stages.remove(stage)

    def run(count, clear):
        together(score(0, count, clear, s0, m0))
        together(score(1, count, clear, s1, m1), weigh(0, count, s0, m0, p0, n0))

        def two(i):
            together(
                gather(2 * i - 2, count, p0, n0),
                score(2 * i, count, clear, s0, m0),
                weigh(2 * i - 1, count, s1, m1, p1, n1),
            )
            together(
                gather(2 * i - 1, count, p1, n1),
                score(2 * i + 1, count, clear, s1, m1),
                weigh(2 * i, count, s0, m0, p0, n0),
            )

        def more(i, carry):
            for g in (2 * i, 2 * i + 1):
                k_copy(g).wait()
                vt_copy(g - 2).wait()
                out_copy(g - 4).start()

            two(i)
            return carry

        steps = groups // 2
        two(1)
        lax.fori_loop(2, steps, more, 0)
        out_copy(groups - 4).start()
        out_copy(groups - 3).start()
        vt_copy(groups - 2).wait()
        vt_copy(groups - 1).wait()
        together(gather(groups - 2, count, p0, n0), weigh(groups - 1, count, s1, m1, p1, n1))
        out_copy(groups - 2).start()
        together(gather(groups - 1, count, p1, n1))
        out_copy(groups - 1).start()
        for g in range(groups):
            out_copy(g).wait()

    most = (blocks - 1) * LANES

    @pl.when(used <= 0)
    def _():
        for pair in range(2 * groups):
            put(pair, jnp.zeros((half, LANES), F32), jnp.full((1, LANES), EMPTY, F32))
        for g in range(groups):
            out_copy(g).start()
        for g in range(4, groups + 2):
            if g < groups:
                k_copy(g).wait()
            vt_copy(g - 2).wait()
        for g in range(groups):
            out_copy(g).wait()

    @pl.when((used > 0) & (used <= most))
    def _():
        run(blocks - 1, 0)

    @pl.when(used > most)
    def _():
        run(blocks, blocks - 1)


def output_kernel(rep_ref, part_ref, *refs):
    weights, out_ref = refs[:-1], refs[-1]
    segs = part_ref.shape[0]
    half = part_ref.shape[1] - STAT_ROWS
    log_sum = jnp.sum(part_ref[:, half : half + STAT_ROWS, :].astype(F32), axis=1)
    share = jnp.exp2(log_sum - jnp.max(log_sum, axis=0, keepdims=True))
    share = share / jnp.sum(share, axis=0, keepdims=True)
    total = jnp.zeros((half, LANES), F32)
    for j in range(segs):
        total += part_ref[j, 0:half, :].astype(F32) * share[j : j + 1, :]
    attended = flip_pair(total).astype(BF16)
    each = segs // len(weights)
    for i, w_ref in enumerate(weights):
        first = (rep_ref[0] ^ i) * each
        update = jnp.dot(attended, w_ref[...], preferred_element_type=F32)
        for j in range(each):
            out_ref[(first + j) ^ FIRST] = update[:, j * LANES : (j + 1) * LANES].astype(BF16)


def sum_kernel(part_ref, out_ref):
    total = part_ref[0].astype(F32)
    for j in range(1, part_ref.shape[0]):
        total += part_ref[j].astype(F32)
    out_ref[...] = total.astype(BF16)


CORE = [(0, 1), (1, 0), (2, 3), (3, 2)]
CHIP = [(0, 2), (1, 3), (2, 0), (3, 1)]


def over_rep(block):
    far = lax.ppermute(block, "rep", CHIP)
    near = lax.ppermute(block, "rep", CORE)
    both = lax.ppermute(far, "rep", CORE)
    return block, near, far, both


def swapped(blocks):
    order = [[j ^ FIRST for j in range(blocks.shape[0])]]
    return lax.all_to_all(
        blocks, "seg", split_axis=0, concat_axis=0, tiled=True, axis_index_groups=order
    )


def sublayer(
    decoder_rows,
    norm_gain,
    query_weight,
    key_codes,
    key_scale,
    value_codes,
    value_scale,
    enc_lengths,
    output_weight,
):
    segs = lax.axis_size("seg")
    rows, own = decoder_rows.shape
    _, tokens, inner = key_codes.shape
    _, heads = key_scale.shape[1:]
    head_dim = inner // heads
    rep = lax.axis_index("rep").astype(jnp.int32).reshape(1)
    used = jnp.clip(enc_lengths - lax.axis_index("seg") * tokens, 0, tokens).astype(jnp.int32)
    gain = norm_gain.reshape(segs, own)
    key_lanes = jnp.repeat(key_scale[0] * LOG2E, head_dim, axis=1)
    value_logs = jnp.repeat(jnp.log2(value_scale[0]), head_dim, axis=1)
    value_inverse = jnp.repeat(1.0 / value_scale[0], head_dim, axis=1)

    wq, wq_near, wq_far, wq_both = over_rep(query_weight)
    x_all = swapped(jnp.broadcast_to(decoder_rows[None], (segs, rows, own)))
    groups, wide = inner // (2 * LANES), 2 * LANES
    height = LANES + SUM_ROWS
    steps = 4
    turn_call = pl.pallas_call(
        turn_kernel,
        grid=(steps,),
        out_shape=(
            jax.ShapeDtypeStruct((groups, 2, height, tokens), BF16),
            jax.ShapeDtypeStruct((4, tokens, wide), BF16),
            jax.ShapeDtypeStruct((2, 2, height, tokens), BF16),
        ),
        in_specs=[
            pl.BlockSpec((tokens, inner // steps), lambda i: (0, i)),
            pl.BlockSpec((tokens, 4 * wide), lambda i: (0, 0)),
        ],
        out_specs=(
            pl.BlockSpec((groups // steps, 2, height, tokens), lambda i: (i, 0, 0, 0)),
            pl.BlockSpec((4, tokens, wide), lambda i: (0, 0, 0)),
            pl.BlockSpec((2, 2, height, tokens), lambda i: (0, 0, 0, 0)),
        ),
        compiler_params=params(51),
        cost_estimate=cost(2 * inner * tokens * 512, 8 << 20),
        name="turn",
    )
    values_t, first_keys, first_values = turn_call(value_codes[0], key_codes[0])

    stage_call = pl.pallas_call(
        stage_kernel,
        out_shape=(
            jax.ShapeDtypeStruct(wq.shape, BF16),
            jax.ShapeDtypeStruct(gain.shape, F32),
        ),
        in_specs=[VMEM] * 2,
        out_specs=(VMEM, VMEM),
        compiler_params=params(8),
        cost_estimate=cost(1 << 24, 1 << 20),
        name="stage",
    )
    wq, gain = stage_call(wq, gain)
    query_call = pl.pallas_call(
        query_kernel,
        out_shape=jax.ShapeDtypeStruct((segs, head_dim, LANES), BF16),
        in_specs=[SMEM] + [VMEM] * 6,
        out_specs=VMEM,
        compiler_params=params(16),
        cost_estimate=cost(2 * rows * inner * own, 2 << 20),
        name="query",
    )
    x_all, key_lanes, value_logs, value_inverse = lax.optimization_barrier(
        (x_all, key_lanes, value_logs, value_inverse)
    )
    query_sent = query_call(rep, x_all, gain, wq, wq_near, wq_far, wq_both)
    queries = swapped(query_sent)

    parts = pl.pallas_call(
        attend_kernel,
        out_shape=jax.ShapeDtypeStruct((segs, head_dim + STAT_ROWS, LANES), BF16),
        in_specs=[SMEM] + [VMEM] * 6 + [HBM] * 2,
        out_specs=HBM,
        scratch_shapes=[
            pltpu.VMEM((segs, head_dim + STAT_ROWS, LANES), BF16),
            pltpu.VMEM((groups, tokens, wide), BF16),
            pltpu.VMEM((groups, 2, height, tokens), BF16),
        ]
        + [pltpu.VMEM((tokens, wide), F32)] * 2
        + [pltpu.VMEM((tokens, wide), BF16)] * 2
        + [pltpu.VMEM((1, wide), F32)] * 4
        + [pltpu.SemaphoreType.DMA((groups,))] * 3,
        compiler_params=params(51),
        cost_estimate=cost(16 * rows * inner * tokens, 9 << 20),
        name="attend",
    )(used, queries, key_lanes, value_logs, value_inverse, first_keys, first_values, key_codes[0], values_t)
    parts = swapped(parts)

    output_blocks = over_rep(output_weight)
    sent = pl.pallas_call(
        output_kernel,
        out_shape=jax.ShapeDtypeStruct((segs, rows, own), BF16),
        in_specs=[SMEM] + [VMEM] * 5,
        out_specs=VMEM,
        compiler_params=params(16),
        cost_estimate=cost(2 * rows * inner * own, 2 << 20),
        name="output",
    )(rep, parts, *output_blocks)
    return pl.pallas_call(
        sum_kernel,
        out_shape=jax.ShapeDtypeStruct((rows, own), BF16),
        in_specs=[VMEM],
        out_specs=VMEM,
        compiler_params=params(8),
        name="gather_sum",
    )(swapped(sent))


def solution(mesh):
    placed = (
        P("rep", "seg"),
        P(),
        P("rep", "seg"),
        P("rep", "seg", None),
        P("rep", "seg", None),
        P("rep", "seg", None),
        P("rep", "seg", None),
        P("rep"),
        P("seg", "rep"),
    )
    return jax.shard_map(
        sublayer, mesh=mesh, in_specs=placed, out_specs=P("rep", "seg"), check_vma=False
    )
```
